32 devices in a mesh: dom: 16 (over z, y, x), mp: 2 (over core).
Axes of the slice: x: 2, y: 2, z: 4, core: 2. Of those that a mesh axis runs over, the one named last changes fastest.
Arguments:
- table: bfloat16 [65536, 768], P('dom', 'mp'), may hold values from -6 to 6
- weight_a: bfloat16 [1536, 512], P(None, 'mp'), may hold values from -0.15625 to 0.15625
- bias_a: float32 [512], replicated, may hold values from -3 to 3
- weight_b: bfloat16 [1024, 512], P(None, 'mp'), may hold values from -0.25 to 0.25
- bias_b: float32 [512], replicated, may hold values from -3 to 3
- requests: int32 [16, 16, 128], P('dom'), may hold values from 0 to 4095
- near_a: int32 [16384, 10], P('dom'), may hold values from 0 to 2047
- self_a: int32 [16384], P('dom'), may hold values from 0 to 2047
- count_a: int32 [16384], P('dom'), may hold values from 1 to 10
- near_b: int32 [4096, 5], P('dom'), may hold values from 0 to 1023
- self_b: int32 [4096], P('dom'), may hold values from 0 to 1023
- count_b: int32 [4096], P('dom'), may hold values from 1 to 5
Outputs:
- embedding: bfloat16 [4096, 512], P('dom', 'mp')
The draws below stay inside these ranges and needn't reach their ends.
Inputs may be any that keep to these rules, and one draw needn't show every extreme that they name: `requests`: local row indices at the owner. `near_a`: slots of the same minibatch; entries at j >= count_a are padding. `near_b`: positions within the same minibatch; entries at j >= count_b are padding.
All inputs are finite; a program needn't handle non-finite values.
Results may differ from the reference program's by a relative error of at most 0.0074.
Values may be sent and summed in bfloat16 or wider, within the bound.
No kernel may reach another device: no remote copies, remote signals or barrier semaphores. Data moves between devices by JAX's collectives and lax.ppermute only.
A program may use at most 64 MiB of HBM per device.

```python
import jax
import jax.numpy as jnp
from jax import lax

F = 768
H = 512
FAN_A = 10
FAN_B = 5
SEEDS_DEV = 256
NODE_DEV = 4096
HOP_DEV = 1024
SLOTS_DEV = 2048
NODES = 65536
HOPS = 16384
SEEDS = 4096
N_DOM = 16


def set_ends(values, stream_key, smallest, high):
    index_at = [jax.random.randint(jax.random.fold_in(stream_key, axis), (), 0, length) for axis, length in enumerate(values.shape)]
    widest = values.shape.index(max(values.shape))
    beside = index_at[:widest] + [(index_at[widest] + 1) % values.shape[widest]] + index_at[widest + 1:]
    return values.at[tuple(index_at)].set(smallest).at[tuple(beside)].set(high)


def level_of(rng, dims, split, smallest, high):
    def one(axis_at, blocks):
        heights = jax.random.uniform(jax.random.fold_in(jax.random.fold_in(rng, 6), axis_at), (blocks,), jnp.float32, smallest / len(split), high / len(split))
        return jnp.repeat(jnp.exp(heights), dims[axis_at] // blocks).reshape((-1,) + (1,) * (len(dims) - axis_at - 1))

    level = one(*split[0])
    for cut in split[1:]:
        level = level * one(*cut)
    return level


def centred(rng, dims, width, most, shards=(), kind=jnp.bfloat16):
    loudness = level_of(rng, dims, shards, -0.22, 0.18) if shards else 1.0
    values = jax.random.normal(rng, dims, jnp.float32) * width * loudness
    return jnp.minimum(jnp.maximum(values, -most), most).astype(kind)


def setup_inputs(seed: int = 0) -> dict:
    splits = jax.random.split(jax.random.key(seed), 13)
    table = centred(splits[0], (NODES, F), 1.0, 6.0, ((0, 16), (1, 2)))
    weight_a = centred(splits[1], (2 * F, H), (2 * F) ** -0.5, 0.15625, ((1, 2),))
    bias_a = centred(splits[2], (H,), 0.5, 3.0, (), jnp.float32)
    weight_b = centred(splits[3], (2 * H, H), H ** -0.5, 0.25, ((1, 2),))
    bias_b = centred(splits[4], (H,), 0.5, 3.0, (), jnp.float32)
    requests = set_ends(jax.random.randint(splits[5], (N_DOM, N_DOM, SLOTS_DEV // N_DOM), 0, NODE_DEV), jax.random.fold_in(splits[5], 1), 0, NODE_DEV - 1).astype(jnp.int32)
    near_a = set_ends(jax.random.randint(splits[6], (HOPS, FAN_A), 0, SLOTS_DEV), jax.random.fold_in(splits[6], 1), 0, SLOTS_DEV - 1).astype(jnp.int32)
    self_a = set_ends(jax.random.randint(splits[7], (HOPS,), 0, SLOTS_DEV), jax.random.fold_in(splits[7], 1), 0, SLOTS_DEV - 1).astype(jnp.int32)
    count_a = set_ends(jax.random.randint(splits[8], (HOPS,), 1, FAN_A + 1), jax.random.fold_in(splits[8], 1), 1, FAN_A).astype(jnp.int32)
    near_b = set_ends(jax.random.randint(splits[9], (SEEDS, FAN_B), 0, HOP_DEV), jax.random.fold_in(splits[9], 1), 0, HOP_DEV - 1).astype(jnp.int32)
    self_b = set_ends(jax.random.randint(splits[10], (SEEDS,), 0, HOP_DEV), jax.random.fold_in(splits[10], 1), 0, HOP_DEV - 1).astype(jnp.int32)
    count_b = set_ends(jax.random.randint(splits[11], (SEEDS,), 1, FAN_B + 1), jax.random.fold_in(splits[11], 1), 1, FAN_B).astype(jnp.int32)
    return {"table": table, "weight_a": weight_a, "bias_a": bias_a, "weight_b": weight_b, "bias_b": bias_b, "requests": requests, "near_a": near_a, "self_a": self_a, "count_a": count_a, "near_b": near_b, "self_b": self_b, "count_b": count_b}


def mean_rows(source, neighbours, counts):
    running = jnp.zeros((neighbours.shape[0], source.shape[1]), jnp.float32)
    for column in range(neighbours.shape[1]):
        keep_mask = (counts > column)[:, None]
        running = running + jnp.where(keep_mask, source[neighbours[:, column]].astype(jnp.float32), 0.0)
    return (running / counts[:, None].astype(jnp.float32)).astype(jnp.bfloat16)

def reference(table, weight_a, bias_a, weight_b, bias_b, requests, near_a, self_a, count_a, near_b, self_b, count_b):
    offsets = (jnp.arange(N_DOM) * NODE_DEV).astype(jnp.int32)[:, None]

    def per_device(blocks):
        asked, hop_near, hop_self, hop_count, seed_near, seed_self, seed_count = blocks
        row_ids = (asked + offsets).reshape(-1).astype(jnp.int32)
        fetched = table[row_ids]
        mean_a = mean_rows(fetched, hop_near, hop_count)
        inputs_a = jnp.concatenate([fetched[hop_self], mean_a], axis=1)
        before = jnp.dot(inputs_a, weight_a, preferred_element_type=jnp.float32) + bias_a
        hidden_a = jax.nn.relu(before).astype(jnp.bfloat16)
        mean_b = mean_rows(hidden_a, seed_near, seed_count)
        inputs_b = jnp.concatenate([hidden_a[seed_self], mean_b], axis=1)
        state = jax.nn.relu(jnp.dot(inputs_b, weight_b, preferred_element_type=jnp.float32) + bias_b)
        squares = lax.optimization_barrier(jnp.sum(state * state, axis=1, keepdims=True))
        return (state * jnp.sqrt(jnp.float32(H)) / jnp.sqrt(squares + H)).astype(jnp.bfloat16)
    blocks = (requests, near_a.reshape(N_DOM, HOP_DEV, FAN_A), self_a.reshape(N_DOM, HOP_DEV), count_a.reshape(N_DOM, HOP_DEV), near_b.reshape(N_DOM, SEEDS_DEV, FAN_B), self_b.reshape(N_DOM, SEEDS_DEV), count_b.reshape(N_DOM, SEEDS_DEV))
    result = lax.map(per_device, blocks)
    return result.reshape(N_DOM * SEEDS_DEV, H)
```

```python
import functools

import jax
import jax.numpy as jnp
from jax import lax
from jax.experimental import pallas as pl
from jax.sharding import PartitionSpec as P


LANES = 128
ROWS = 32


def spans_of(per):
    return ((0, per),)


def split_index(value, size):
    if size & (size - 1) == 0:
        return lax.shift_right_logical(value, size.bit_length() - 1), value & (size - 1)
    quotient = lax.div(value, size)
    return quotient, value - quotient * size


def place_of(slots, per, owners, spans):
    owner, row = split_index(slots, per)
    place = jnp.zeros_like(slots)
    for low, high in spans:
        inside = (row >= low) & (row < high)
        place = jnp.where(inside, owners * low + owner * (high - low) + row - low, place)
    return place


def fill_counts(tab_ref, fan, place_fn, outs):
    total = tab_ref.shape[0]
    bits = max(1, fan.bit_length())
    fields = 32 // bits
    blocks = [(ref, at) for ref in outs for at in range(ref.shape[2] // LANES)]
    words = -(-len(blocks) // fields)
    rows = min(ROWS, total)
    lanes = lax.broadcasted_iota(jnp.int32, (rows, LANES), 1)
    column = lax.broadcasted_iota(jnp.int32, (rows, fan + 1), 1)

    def step(index, carry):
        at = pl.multiple_of(index * rows, rows)
        here = pl.ds(at, rows)
        piece = tab_ref[here, :]
        place = place_fn(piece[:, : fan + 1])
        block, low = split_index(place, LANES)
        valid = column < piece[:, fan + 1 : fan + 2]
        word, field = split_index(block, fields)
        unit = jnp.where(valid, jnp.left_shift(jnp.ones_like(field), field * bits), 0)
        units = [jnp.where(word == w, unit, 0) for w in range(words)]
        sums = [jnp.zeros((rows, LANES), jnp.int32) for _ in range(words)]
        for j in range(fan):
            hit = lanes == low[:, j : j + 1]
            for w in range(words):
                sums[w] = sums[w] + jnp.where(hit, units[w][:, j : j + 1], 0)
        own = place[:, fan : fan + 1]
        for number, (ref, part) in enumerate(blocks):
            count = lax.shift_right_logical(sums[number // fields], bits * (number % fields))
            count = (count & ((1 << bits) - 1)).astype(jnp.float32)
            cols = slice(part * LANES, (part + 1) * LANES)
            ref[0, here, cols] = count.astype(jnp.bfloat16)
            one = jnp.where(lanes + number * LANES == own, 1.0, 0.0)
            ref[1, here, cols] = one.astype(jnp.bfloat16)
        return carry

    lax.fori_loop(0, total // rows, step, 0)


def count_matrices(tab, fan, place_fn, widths):
    total = tab.shape[0]

    def body(tab_ref, *outs):
        fill_counts(tab_ref, fan, place_fn, outs)

    return pl.pallas_call(
        body,
        out_shape=[jax.ShapeDtypeStruct((2, total, width), jnp.bfloat16) for width in widths],
        cost_estimate=pl.CostEstimate(flops=10**9, bytes_accessed=10**7, transcendentals=0),
    )(tab)


def gather_sums(counts, rows, before):
    hops = counts.shape[1]
    width = counts.shape[2]
    cols = rows.shape[1]
    block = min(256, hops)

    def body(*refs):
        c_ref, x_ref = refs[0], refs[1]
        o_ref = refs[-1]
        value = jnp.dot(c_ref[...].reshape(2 * block, width), x_ref[...], preferred_element_type=jnp.float32)
        if before is not None:
            value = value + refs[2][...].reshape(2 * block, cols)
        o_ref[...] = value.reshape(2, block, cols)

    acc_spec = pl.BlockSpec((2, block, cols), lambda i: (0, i, 0))
    specs = [pl.BlockSpec((2, block, width), lambda i: (0, i, 0)), pl.BlockSpec((width, cols), lambda i: (0, 0))]
    operands = [counts, rows]
    if before is not None:
        specs.append(acc_spec)
        operands.append(before)
    return pl.pallas_call(
        body,
        grid=(hops // block,),
        in_specs=specs,
        out_specs=acc_spec,
        out_shape=jax.ShapeDtypeStruct((2, hops, cols), jnp.float32),
        cost_estimate=pl.CostEstimate(flops=4 * hops * width * cols, bytes_accessed=10**7, transcendentals=0),
        name="gather_sums",
    )(*operands)


def first_layer(counts, rows, before, count_a, weight):
    hops = counts.shape[1]
    width = counts.shape[2]
    cols = rows.shape[1]
    hidden = weight.shape[2]
    block = min(256, hops)

    def body(*refs):
        c_ref, x_ref, n_ref, w_ref = refs[:4]
        o_ref, s_ref = refs[-2:]
        value = jnp.dot(c_ref[...].reshape(2 * block, width), x_ref[...], preferred_element_type=jnp.float32)
        value = value.reshape(2, block, cols)
        if before is not None:
            value = value + refs[4][...]
        own = value[1].astype(jnp.bfloat16)
        mean = (value[0] / n_ref[...].astype(jnp.float32)).astype(jnp.bfloat16)
        out = jnp.dot(own, w_ref[0], preferred_element_type=jnp.float32)
        out = out + jnp.dot(mean, w_ref[1], preferred_element_type=jnp.float32)
        o_ref[...] = out
        s_ref[...] = out.astype(jnp.bfloat16)

    specs = [
        pl.BlockSpec((2, block, width), lambda i: (0, i, 0)),
        pl.BlockSpec((width, cols), lambda i: (0, 0)),
        pl.BlockSpec((block, 1), lambda i: (i, 0)),
        pl.BlockSpec((2, cols, hidden), lambda i: (0, 0, 0)),
    ]
    operands = [counts, rows, count_a, weight]
    if before is not None:
        specs.append(pl.BlockSpec((2, block, cols), lambda i: (0, i, 0)))
        operands.append(before)
    out_spec = pl.BlockSpec((block, hidden), lambda i: (i, 0))
    return pl.pallas_call(
        body,
        grid=(hops // block,),
        in_specs=specs,
        out_specs=[out_spec, out_spec],
        out_shape=[
            jax.ShapeDtypeStruct((hops, hidden), jnp.float32),
            jax.ShapeDtypeStruct((hops, hidden), jnp.bfloat16),
        ],
        cost_estimate=pl.CostEstimate(flops=4 * hops * width * cols, bytes_accessed=10**7, transcendentals=0),
        name="first_layer",
    )(*operands)


def second_layer(own, other, bias_a, counts, count_b, weight, bias_b):
    hops, hidden = own.shape
    half = hidden // 2
    seeds = counts.shape[1]

    def body(own_ref, other_ref, ba_ref, c_ref, n_ref, w_ref, bb_ref, o_ref):
        other_value = other_ref[...].astype(jnp.float32)
        turned = jnp.concatenate([other_value[:, half:], other_value[:, :half]], axis=1)
        value = own_ref[...] + turned + ba_ref[...]
        value = jnp.maximum(value, 0.0).astype(jnp.bfloat16)
        picked = jnp.dot(c_ref[...].reshape(2 * seeds, hops), value, preferred_element_type=jnp.float32)
        self_b = picked[seeds:].astype(jnp.bfloat16)
        mean_b = (picked[:seeds] / n_ref[...].astype(jnp.float32)).astype(jnp.bfloat16)
        state = jnp.dot(self_b, w_ref[0], preferred_element_type=jnp.float32)
        state = state + jnp.dot(mean_b, w_ref[1], preferred_element_type=jnp.float32)
        state = jnp.maximum(state + bb_ref[...], 0.0)
        squares = jnp.sum(state * state, axis=1, keepdims=True)
        mine = state[:, :half] * jnp.sqrt(jnp.float32(hidden)) / jnp.sqrt(squares + hidden)
        o_ref[...] = mine.astype(jnp.bfloat16)

    return pl.pallas_call(
        body,
        out_shape=jax.ShapeDtypeStruct((seeds, half), jnp.bfloat16),
        cost_estimate=pl.CostEstimate(flops=10**9, bytes_accessed=10**7, transcendentals=0),
        name="second_layer",
    )(own, other, bias_a, counts, count_b, weight, bias_b)


def shards(
    n_dom,
    table,
    weight_a,
    bias_a,
    weight_b,
    bias_b,
    requests,
    near_a,
    self_a,
    count_a,
    near_b,
    self_b,
    count_b,
):
    features = table.shape[1]
    half = weight_a.shape[1]
    per = requests.shape[2]
    mine = lax.axis_index("mp")
    pair = 1 - mine
    swap = [(0, 1), (1, 0)]
    spans = spans_of(per)

    asked = lax.all_to_all(requests[0], "dom", split_axis=0, concat_axis=0, tiled=True)

    place_fn = functools.partial(place_of, per=per, owners=n_dom, spans=spans)
    widths = [n_dom * (high - low) for low, high in spans]
    tab_a = jnp.concatenate([near_a, self_a[:, None], count_a[:, None]], axis=1)
    counts = count_matrices(tab_a, near_a.shape[1], place_fn, widths)
    tab_b = jnp.concatenate([near_b, self_b[:, None], count_b[:, None]], axis=1)
    (counts_b,) = count_matrices(tab_b, near_b.shape[1], lambda value: value, [near_a.shape[0]])

    arrived = []
    for low, high in spans:
        found = table[asked[:, low:high]]
        moved = lax.all_to_all(found, "dom", split_axis=0, concat_axis=0, tiled=True)
        arrived.append(moved.reshape(-1, features))

    split_a = weight_a.reshape(2, 2, features, half)
    mine_a = lax.dynamic_index_in_dim(split_a, mine, 1, keepdims=False)
    send_a = lax.dynamic_index_in_dim(split_a, pair, 1, keepdims=False)
    whole_a = jnp.concatenate([mine_a, lax.ppermute(send_a, "mp", swap)], axis=2)

    def turned(value):
        value = value.reshape((-1, 2, half) + value.shape[1:])
        first = lax.dynamic_index_in_dim(value, mine, 1)
        second = lax.dynamic_index_in_dim(value, pair, 1)
        return jnp.concatenate([first, second], axis=1)

    all_b = jnp.concatenate([weight_b, lax.ppermute(weight_b, "mp", swap)], axis=1)
    whole_b = turned(all_b).reshape(2, 2 * half, 2 * half)
    whole_bias_a = turned(bias_a).reshape(1, 2 * half)
    whole_bias_b = turned(bias_b).reshape(1, 2 * half)

    tail = (whole_a, whole_b, whole_bias_a, whole_bias_b, counts_b, count_a[:, None], count_b[:, None])
    arrived, tail = lax.optimization_barrier((arrived, tail))
    whole_a, whole_b, whole_bias_a, whole_bias_b, counts_b, count_a, count_b = tail

    before = None
    for number in range(len(spans) - 1):
        before = gather_sums(counts[number], arrived[number], before)
    own, send = first_layer(counts[-1], arrived[-1], before, count_a, whole_a)
    other = lax.ppermute(send, "mp", swap)
    return second_layer(own, other, whole_bias_a, counts_b, count_b, whole_b, whole_bias_b)


def solution(mesh):
    placed = (
        P("dom", "mp"),
        P(None, "mp"),
        P(),
        P(None, "mp"),
        P(),
        P("dom", None, None),
        P("dom", None),
        P("dom"),
        P("dom"),
        P("dom", None),
        P("dom"),
        P("dom"),
    )
    return jax.shard_map(
        functools.partial(shards, mesh.shape["dom"]),
        mesh=mesh,
        in_specs=placed,
        out_specs=P("dom", "mp"),
        check_vma=False,
    )
```

```python
import functools

import jax
import jax.numpy as jnp
from jax import lax
from jax.experimental import pallas as pl
from jax.experimental.pallas import tpu as pltpu
from jax.sharding import PartitionSpec as P


LANES = 128
PICK = 2048
BATCHES = ((8, 13), (0, 1, 4, 5, 9, 12))


def split_index(value, size):
    if size & (size - 1) == 0:
        return lax.shift_right_logical(value, size.bit_length() - 1), value & (size - 1)
    quotient = lax.div(value, size)
    return quotient, value - quotient * size


def estimate(flops):
    return pl.CostEstimate(flops=flops, bytes_accessed=10**7, transcendentals=0)


def count_matrices(near, own, count, me, place_fn, widths):
    fan, total = near.shape
    block = min(2 * LANES, total)
    bits = max(1, fan.bit_length())
    fields = 32 // bits
    tall = min(LANES // 2, min(widths))

    def body(me_ref, near_ref, own_ref, count_ref, *outs):
        pieces = [(ref, at) for ref in outs for at in range(ref.shape[1] // LANES)]
        words = -(-len(pieces) // fields)
        rank = lax.broadcasted_iota(jnp.int32, (fan, LANES), 0)
        for lane in range(block // LANES):
            cols = slice(lane * LANES, (lane + 1) * LANES)
            place = place_fn(near_ref[:, cols], me_ref)
            group, low = split_index(place, LANES)
            word, field = split_index(group, fields)
            unit = jnp.left_shift(jnp.ones_like(field), field * bits)
            unit = jnp.where((rank < count_ref[:, cols]) & (place >= 0), unit, 0)
            units = [jnp.where(word == w, unit, 0) for w in range(words)]
            mine = place_fn(own_ref[:, cols], me_ref)
            for top in range(0, LANES, tall):
                rows = lax.broadcasted_iota(jnp.int32, (tall, LANES), 0) + top
                sums = [jnp.zeros((tall, LANES), jnp.int32) for _ in range(words)]
                for j in range(fan):
                    hit = rows == low[j : j + 1, :]
                    for w in range(words):
                        sums[w] = sums[w] + jnp.where(hit, units[w][j : j + 1, :], 0)
                for number, (ref, part) in enumerate(pieces):
                    found = lax.shift_right_logical(sums[number // fields], bits * (number % fields))
                    found = (found & ((1 << bits) - 1)).astype(jnp.float32)
                    here = slice(part * LANES + top, part * LANES + top + tall)
                    ref[0, here, cols] = found.astype(jnp.bfloat16)
                    one = jnp.where(rows == mine - number * LANES, 1.0, 0.0)
                    ref[1, here, cols] = one.astype(jnp.bfloat16)

    line = pl.BlockSpec((1, block), lambda i: (0, i))
    return pl.pallas_call(
        body,
        grid=(total // block,),
        in_specs=[
            pl.BlockSpec(memory_space=pltpu.SMEM),
            pl.BlockSpec((fan, block), lambda i: (0, i)),
            line,
            line,
        ],
        out_specs=[pl.BlockSpec((2, width, block), lambda i: (0, 0, i)) for width in widths],
        out_shape=[jax.ShapeDtypeStruct((2, width, total), jnp.bfloat16) for width in widths],
        cost_estimate=estimate(10**9),
    )(me, near, own, count)


def pick_rows(asked, where, table, their_table, distances, step):
    nodes, share = table.shape
    per = asked.shape[1]
    block = min(PICK, nodes)
    total = len(distances) * per

    def body(at_ref, ask_ref, mine_ref, their_ref, *refs):
        outs, acc, ids = refs[:-2], refs[-2], refs[-1]
        now = pl.program_id(0)

        @pl.when(now == 0)
        def _():
            acc[...] = jnp.zeros_like(acc)
            for number, base in enumerate(distances):
                partner = at_ref[0] ^ (base ^ (step * at_ref[1]))
                line = ask_ref[pl.ds(partner, 1), :]
                ids[number * per : (number + 1) * per, :] = jnp.broadcast_to(line, (LANES, per)).T

        lanes = lax.broadcasted_iota(jnp.int32, (total, LANES), 1) + now * block
        wanted = ids[...]
        marks = [
            jnp.where(wanted - at == lanes, 1.0, 0.0).astype(jnp.bfloat16) for at in range(0, block, LANES)
        ]
        marks = jnp.concatenate(marks, axis=1)
        table_rows = jnp.concatenate([mine_ref[...], their_ref[...]], axis=1)
        acc[...] += jnp.dot(marks, table_rows, preferred_element_type=jnp.float32)

        @pl.when(now == pl.num_programs(0) - 1)
        def _():
            for number, ref in enumerate(outs):
                ref[...] = acc[number * per : (number + 1) * per, :].astype(jnp.bfloat16)

    rows = pl.BlockSpec((block, share), lambda i: (i, 0))
    return pl.pallas_call(
        body,
        grid=(nodes // block,),
        in_specs=[
            pl.BlockSpec(memory_space=pltpu.SMEM),
            pl.BlockSpec(asked.shape, lambda i: (0, 0)),
            rows,
            rows,
        ],
        out_specs=[pl.BlockSpec((per, 2 * share), lambda i: (0, 0))] * len(distances),
        out_shape=[jax.ShapeDtypeStruct((per, 2 * share), jnp.bfloat16)] * len(distances),
        scratch_shapes=[pltpu.VMEM((total, 2 * share), jnp.float32), pltpu.VMEM((total, LANES), jnp.int32)],
        cost_estimate=estimate(4 * total * nodes * share),
    )(where, asked, table, their_table)


def first_layer(counts, count, rows, core, weight, their_weight, before=None, last=False):
    _, width, total = counts.shape
    cols = rows[0].shape[1]
    features, half = weight.shape[0] // 2, weight.shape[1]
    share = cols if cols < features else features // 2
    block = min(2 * LANES, total)
    have = before is not None

    def body(core_ref, c_ref, n_ref, *refs):
        refs = list(refs)
        row_refs = [refs.pop(0) for _ in rows]
        shard_refs = (refs.pop(0), refs.pop(0))
        old_ref = refs.pop(0) if have else None
        o_ref, turned = refs

        @pl.when(pl.program_id(0) == 0)
        def _():
            core_value = core_ref[0]
            first = pl.multiple_of(core_value * share, LANES)
            second = pl.multiple_of((1 - core_value) * share, LANES)
            spots = (first, second) if cols > share else (first,)
            value = jnp.concatenate([ref[...] for ref in row_refs], axis=0)
            for number, ref in enumerate(shard_refs):
                hidden_at = core_value * half if number == 0 else (1 - core_value) * half
                here = pl.ds(pl.multiple_of(hidden_at, LANES), half)
                for part in range(2):
                    pieces = [ref[pl.ds(part * features + at, share), :] for at in spots]
                    piece = jnp.concatenate(pieces, axis=0)
                    product = jnp.dot(value, piece, preferred_element_type=jnp.float32)
                    turned[part, here, :] = product.astype(jnp.bfloat16).T

        out = jnp.dot(turned[1], c_ref[0], preferred_element_type=jnp.float32)
        out = out * (1.0 / n_ref[...].astype(jnp.float32))
        out = out + jnp.dot(turned[0], c_ref[1], preferred_element_type=jnp.float32)
        if have:
            out = out + old_ref[...]
        o_ref[...] = out.astype(o_ref.dtype)

    out_spec = pl.BlockSpec((2 * half, block), lambda i: (0, i))
    specs = [
        pl.BlockSpec(memory_space=pltpu.SMEM),
        pl.BlockSpec((2, width, block), lambda i: (0, 0, i)),
        pl.BlockSpec((1, block), lambda i: (0, i)),
    ]
    specs += [pl.BlockSpec(piece.shape, lambda i: (0, 0)) for piece in rows]
    specs += [pl.BlockSpec(weight.shape, lambda i: (0, 0))] * 2
    operands = [core, counts, count, *rows, weight, their_weight]
    if have:
        specs.append(out_spec)
        operands.append(before)
    return pl.pallas_call(
        body,
        grid=(total // block,),
        in_specs=specs,
        out_specs=out_spec,
        out_shape=jax.ShapeDtypeStruct((2 * half, total), jnp.bfloat16 if last else jnp.float32),
        scratch_shapes=[pltpu.VMEM((2, 2 * half, width), jnp.bfloat16)],
        cost_estimate=estimate(4 * width * total * cols),
    )(*operands)


def second_layer(own, other, bias_a, counts, count, core, weight, their_weight, bias_b):
    hidden, _ = own.shape
    half = hidden // 2
    seeds = counts.shape[2]

    def body(core_ref, own_ref, other_ref, ba_ref, c_ref, n_ref, w_ref, t_ref, bb_ref, o_ref):
        bias = jnp.broadcast_to(ba_ref[...], (LANES, hidden)).T[:, :1]
        value = own_ref[...].astype(jnp.float32) + other_ref[...].astype(jnp.float32) + bias
        value = jnp.maximum(value, 0.0).astype(jnp.bfloat16)
        self_b = jnp.dot(value, c_ref[1], preferred_element_type=jnp.float32)
        mean_b = jnp.dot(value, c_ref[0], preferred_element_type=jnp.float32)
        mean_b = mean_b * (1.0 / n_ref[...].astype(jnp.float32))
        self_b = self_b.T.astype(jnp.bfloat16)
        mean_b = mean_b.T.astype(jnp.bfloat16)

        def state_of(ref, index):
            state = jnp.dot(self_b, ref[:hidden, :], preferred_element_type=jnp.float32)
            state = state + jnp.dot(mean_b, ref[hidden:, :], preferred_element_type=jnp.float32)
            return jnp.maximum(state + bb_ref[pl.ds(index, 1), :], 0.0)

        state = state_of(w_ref, core_ref[0])
        theirs = state_of(t_ref, 1 - core_ref[0])
        squares = jnp.sum(state * state + theirs * theirs, axis=1, keepdims=True)
        scale = jnp.sqrt(jnp.float32(hidden)) / jnp.sqrt(squares + hidden)
        o_ref[...] = (state * scale).astype(jnp.bfloat16)

    whole = pl.BlockSpec(memory_space=pltpu.VMEM)
    return pl.pallas_call(
        body,
        in_specs=[pl.BlockSpec(memory_space=pltpu.SMEM)] + [whole] * 8,
        out_shape=jax.ShapeDtypeStruct((seeds, half), jnp.bfloat16),
        cost_estimate=estimate(10**9),
        name="second_layer",
    )(core, own, other, bias_a, counts, count, weight, their_weight, bias_b)


def plan_of(n_dom):
    if n_dom != 16:
        return None
    return n_dom // 8, (8, 13, 0, 1), (4, 5, 9, 12)


def shards(
    n_dom,
    table,
    weight_a,
    bias_a,
    weight_b,
    bias_b,
    requests,
    near_a,
    self_a,
    count_a,
    near_b,
    self_b,
    count_b,
):
    features = table.shape[1]
    half = weight_a.shape[1]
    per = requests.shape[2]
    me = lax.axis_index("dom")
    core = lax.axis_index("mp")
    core_line = core.reshape(1).astype(jnp.int32)
    where = jnp.stack([me, core]).astype(jnp.int32)
    swap = [(0, 1), (1, 0)]
    plan = plan_of(n_dom)

    def place_fn(slots, at_ref):
        if plan is None:
            return slots
        step, early, late = plan
        owner, row = split_index(slots, per)
        distance = owner ^ at_ref[0]
        rank = jnp.full_like(slots, -2 * n_dom)
        for number, base in enumerate(early + late):
            rank = jnp.where(distance == base ^ (step * at_ref[1]), number, rank)
        return rank * per + row

    if plan is not None:
        their_table = lax.ppermute(table, "mp", swap)
    asked = lax.all_to_all(requests[0], "dom", split_axis=0, concat_axis=0, tiled=True)

    widths = [n_dom * per] if plan is None else [len(part) * per for part in plan[1:]]
    if plan is not None:
        near_a, their_table = lax.optimization_barrier((near_a, their_table))
    counts = count_matrices(near_a.T, self_a[None], count_a[None], where, place_fn, widths)
    (counts_b,) = count_matrices(
        near_b.T, self_b[None], count_b[None], where, lambda value, _: value, [near_a.shape[0]]
    )

    if plan is None:
        found = table.at[asked].get(mode="promise_in_bounds")
        moved = lax.all_to_all(found, "dom", split_axis=0, concat_axis=0, tiled=True)
        early, late = [], [moved.reshape(-1, features)]
    else:
        step = plan[0]
        found = {}
        for bases in BATCHES:
            picked = pick_rows(asked, where, table, their_table, bases, step)
            found.update(zip(bases, picked))

        def trade(base):
            pairs = [
                (2 * i + c, 2 * (i ^ (base ^ (step * c))) + c) for i in range(n_dom) for c in range(2)
            ]
            return lax.ppermute(found[base], ("dom", "mp"), pairs)

        early = [trade(base) for base in plan[1]]
        late = [trade(base) for base in plan[2]]

    their_a = lax.ppermute(weight_a, "mp", swap)
    their_b = lax.ppermute(weight_b, "mp", swap)
    count_line = count_a[None]
    before = None
    if early:
        early, (their_a, their_b, counts_b) = lax.optimization_barrier((early, (their_a, their_b, counts_b)))
        before = first_layer(counts[0], count_line, early, core_line, weight_a, their_a)
    own = first_layer(counts[-1], count_line, late, core_line, weight_a, their_a, before, last=True)
    other = lax.ppermute(own, "mp", swap)
    return second_layer(
        own, other, bias_a[None], counts_b, count_b[None], core_line, weight_b, their_b, bias_b.reshape(2, half)
    )


def solution(mesh):
    placed = (
        P("dom", "mp"),
        P(None, "mp"),
        P(),
        P(None, "mp"),
        P(),
        P("dom", None, None),
        P("dom", None),
        P("dom"),
        P("dom"),
        P("dom", None),
        P("dom"),
        P("dom"),
    )
    n_dom = mesh.shape["dom"]
    return jax.shard_map(
        functools.partial(shards, n_dom),
        mesh=mesh,
        in_specs=placed,
        out_specs=P("dom", "mp"),
        check_vma=False,
    )
```

```python
import functools

import jax
import jax.numpy as jnp
from jax import lax
from jax.experimental import pallas as pl
from jax.experimental.pallas import tpu as pltpu
from jax.sharding import PartitionSpec as P


LANES = 128
PICK = 2048
BATCHES = ((8, 13), (0, 1, 4, 5, 9, 12))


def split_index(value, size):
    if size & (size - 1) == 0:
        return lax.shift_right_logical(value, size.bit_length() - 1), value & (size - 1)
    quotient = lax.div(value, size)
    return quotient, value - quotient * size


def estimate(flops):
    return pl.CostEstimate(flops=flops, bytes_accessed=10**7, transcendentals=0)


def count_matrices(near, own, count, me, place_fn, widths):
    fan, total = near.shape
    block = min(2 * LANES, total)
    bits = max(1, fan.bit_length())
    fields = 32 // bits
    tall = min(LANES // 2, min(widths))

    def body(me_ref, near_ref, own_ref, count_ref, *outs):
        pieces = [(ref, at) for ref in outs for at in range(ref.shape[1] // LANES)]
        words = -(-len(pieces) // fields)
        rank = lax.broadcasted_iota(jnp.int32, (fan, LANES), 0)
        for lane in range(block // LANES):
            cols = slice(lane * LANES, (lane + 1) * LANES)
            place = place_fn(near_ref[:, cols], me_ref)
            group, low = split_index(place, LANES)
            word, field = split_index(group, fields)
            unit = jnp.left_shift(jnp.ones_like(field), field * bits)
            unit = jnp.where((rank < count_ref[:, cols]) & (place >= 0), unit, 0)
            units = [jnp.where(word == w, unit, 0) for w in range(words)]
            mine = place_fn(own_ref[:, cols], me_ref)
            for top in range(0, LANES, tall):
                rows = lax.broadcasted_iota(jnp.int32, (tall, LANES), 0) + top
                sums = [jnp.zeros((tall, LANES), jnp.int32) for _ in range(words)]
                for j in range(fan):
                    hit = rows == low[j : j + 1, :]
                    for w in range(words):
                        sums[w] = sums[w] + jnp.where(hit, units[w][j : j + 1, :], 0)
                for number, (ref, part) in enumerate(pieces):
                    found = lax.shift_right_logical(sums[number // fields], bits * (number % fields))
                    found = (found & ((1 << bits) - 1)).astype(jnp.float32)
                    here = slice(part * LANES + top, part * LANES + top + tall)
                    ref[0, here, cols] = found.astype(jnp.bfloat16)
                    one = jnp.where(rows == mine - number * LANES, 1.0, 0.0)
                    ref[1, here, cols] = one.astype(jnp.bfloat16)

    line = pl.BlockSpec((1, block), lambda i: (0, i))
    return pl.pallas_call(
        body,
        grid=(total // block,),
        in_specs=[
            pl.BlockSpec(memory_space=pltpu.SMEM),
            pl.BlockSpec((fan, block), lambda i: (0, i)),
            line,
            line,
        ],
        out_specs=[pl.BlockSpec((2, width, block), lambda i: (0, 0, i)) for width in widths],
        out_shape=[jax.ShapeDtypeStruct((2, width, total), jnp.bfloat16) for width in widths],
        compiler_params=pltpu.CompilerParams(vmem_limit_bytes=None),
        cost_estimate=estimate(10**9),
    )(me, near, own, count)


def pick_rows(asked, where, table, their_table, distances, step):
    nodes, share = table.shape
    per = asked.shape[1]
    block = min(PICK, nodes)
    total = len(distances) * per

    def body(at_ref, ask_ref, mine_ref, their_ref, *refs):
        outs, acc, ids = refs[:-2], refs[-2], refs[-1]
        now = pl.program_id(0)

        @pl.when(now == 0)
        def _():
            acc[...] = jnp.zeros_like(acc)
            for number, base in enumerate(distances):
                partner = at_ref[0] ^ (base ^ (step * at_ref[1]))
                line = ask_ref[pl.ds(partner, 1), :]
                ids[number * per : (number + 1) * per, :] = jnp.broadcast_to(line, (LANES, per)).T

        lanes = lax.broadcasted_iota(jnp.int32, (total, LANES), 1) + now * block
        wanted = ids[...]
        marks = [
            jnp.where(wanted - at == lanes, 1.0, 0.0).astype(jnp.bfloat16) for at in range(0, block, LANES)
        ]
        marks = jnp.concatenate(marks, axis=1)
        table_rows = jnp.concatenate([mine_ref[...], their_ref[...]], axis=1)
        acc[...] += jnp.dot(marks, table_rows, preferred_element_type=jnp.float32)

        @pl.when(now == pl.num_programs(0) - 1)
        def _():
            for number, ref in enumerate(outs):
                ref[...] = acc[number * per : (number + 1) * per, :].astype(jnp.bfloat16)

    rows = pl.BlockSpec((block, share), lambda i: (i, 0))
    return pl.pallas_call(
        body,
        grid=(nodes // block,),
        in_specs=[
            pl.BlockSpec(memory_space=pltpu.SMEM),
            pl.BlockSpec(asked.shape, lambda i: (0, 0)),
            rows,
            rows,
        ],
        out_specs=[pl.BlockSpec((per, 2 * share), lambda i: (0, 0))] * len(distances),
        out_shape=[jax.ShapeDtypeStruct((per, 2 * share), jnp.bfloat16)] * len(distances),
        scratch_shapes=[pltpu.VMEM((total, 2 * share), jnp.float32), pltpu.VMEM((total, LANES), jnp.int32)],
        compiler_params=pltpu.CompilerParams(vmem_limit_bytes=32 * 2**20),
        cost_estimate=estimate(4 * total * nodes * share),
    )(where, asked, table, their_table)


def first_layer(counts, count, rows, core, weight, their_weight, before=None, last=False):
    _, width, total = counts.shape
    cols = rows[0].shape[1]
    features, half = weight.shape[0] // 2, weight.shape[1]
    share = cols if cols < features else features // 2
    block = min(4 * LANES, total)
    have = before is not None

    def body(core_ref, c_ref, n_ref, *refs):
        refs = list(refs)
        row_refs = [refs.pop(0) for _ in rows]
        shard_refs = (refs.pop(0), refs.pop(0))
        old_ref = refs.pop(0) if have else None
        o_ref, turned = refs

        @pl.when(pl.program_id(0) == 0)
        def _():
            core_value = core_ref[0]
            first = pl.multiple_of(core_value * share, LANES)
            second = pl.multiple_of((1 - core_value) * share, LANES)
            spots = (first, second) if cols > share else (first,)
            value = jnp.concatenate([ref[...] for ref in row_refs], axis=0)
            for number, ref in enumerate(shard_refs):
                hidden_at = core_value * half if number == 0 else (1 - core_value) * half
                here = pl.ds(pl.multiple_of(hidden_at, LANES), half)
                for part in range(2):
                    pieces = [ref[pl.ds(part * features + at, share), :] for at in spots]
                    piece = jnp.concatenate(pieces, axis=0)
                    product = jnp.dot(value, piece, preferred_element_type=jnp.float32)
                    turned[part, here, :] = product.astype(jnp.bfloat16).T

        out = jnp.dot(turned[1], c_ref[0], preferred_element_type=jnp.float32)
        out = out * (1.0 / n_ref[...].astype(jnp.float32))
        out = out + jnp.dot(turned[0], c_ref[1], preferred_element_type=jnp.float32)
        if have:
            out = out + old_ref[...]
        o_ref[...] = out.astype(o_ref.dtype)

    out_spec = pl.BlockSpec((2 * half, block), lambda i: (0, i))
    specs = [
        pl.BlockSpec(memory_space=pltpu.SMEM),
        pl.BlockSpec((2, width, block), lambda i: (0, 0, i)),
        pl.BlockSpec((1, block), lambda i: (0, i)),
    ]
    specs += [pl.BlockSpec(piece.shape, lambda i: (0, 0)) for piece in rows]
    specs += [pl.BlockSpec(weight.shape, lambda i: (0, 0))] * 2
    operands = [core, counts, count, *rows, weight, their_weight]
    if have:
        specs.append(out_spec)
        operands.append(before)
    return pl.pallas_call(
        body,
        grid=(total // block,),
        in_specs=specs,
        out_specs=out_spec,
        out_shape=jax.ShapeDtypeStruct((2 * half, total), jnp.bfloat16 if last else jnp.float32),
        scratch_shapes=[pltpu.VMEM((2, 2 * half, width), jnp.bfloat16)],
        compiler_params=pltpu.CompilerParams(vmem_limit_bytes=32 * 2**20),
        cost_estimate=estimate(4 * width * total * cols),
    )(*operands)


def second_layer(own, other, bias_a, counts, count, core, weight, their_weight, bias_b):
    hidden, _ = own.shape
    half = hidden // 2
    seeds = counts.shape[2]

    def body(core_ref, own_ref, other_ref, ba_ref, c_ref, n_ref, w_ref, t_ref, bb_ref, o_ref):
        bias = jnp.broadcast_to(ba_ref[...], (LANES, hidden)).T[:, :1]
        value = own_ref[...].astype(jnp.float32) + other_ref[...].astype(jnp.float32) + bias
        value = jnp.maximum(value, 0.0).astype(jnp.bfloat16)
        self_b = jnp.dot(value, c_ref[1], preferred_element_type=jnp.float32)
        mean_b = jnp.dot(value, c_ref[0], preferred_element_type=jnp.float32)
        mean_b = mean_b * (1.0 / n_ref[...].astype(jnp.float32))
        self_b = self_b.T.astype(jnp.bfloat16)
        mean_b = mean_b.T.astype(jnp.bfloat16)

        def state_of(ref, index):
            state = jnp.dot(self_b, ref[:hidden, :], preferred_element_type=jnp.float32)
            state = state + jnp.dot(mean_b, ref[hidden:, :], preferred_element_type=jnp.float32)
            return jnp.maximum(state + bb_ref[pl.ds(index, 1), :], 0.0)

        state = state_of(w_ref, core_ref[0])
        theirs = state_of(t_ref, 1 - core_ref[0])
        squares = jnp.sum(state * state + theirs * theirs, axis=1, keepdims=True)
        scale = jnp.sqrt(jnp.float32(hidden)) / jnp.sqrt(squares + hidden)
        o_ref[...] = (state * scale).astype(jnp.bfloat16)

    whole = pl.BlockSpec(memory_space=pltpu.VMEM)
    return pl.pallas_call(
        body,
        in_specs=[pl.BlockSpec(memory_space=pltpu.SMEM)] + [whole] * 8,
        out_shape=jax.ShapeDtypeStruct((seeds, half), jnp.bfloat16),
        compiler_params=pltpu.CompilerParams(vmem_limit_bytes=None),
        cost_estimate=estimate(10**9),
        name="second_layer",
    )(core, own, other, bias_a, counts, count, weight, their_weight, bias_b)


def plan_of(n_dom):
    if n_dom != 16:
        return None
    return n_dom // 8, (8, 13, 0), (1, 4, 5, 9, 12)


def shards(
    n_dom,
    table,
    weight_a,
    bias_a,
    weight_b,
    bias_b,
    requests,
    near_a,
    self_a,
    count_a,
    near_b,
    self_b,
    count_b,
):
    features = table.shape[1]
    half = weight_a.shape[1]
    per = requests.shape[2]
    me = lax.axis_index("dom")
    core = lax.axis_index("mp")
    core_line = core.reshape(1).astype(jnp.int32)
    where = jnp.stack([me, core]).astype(jnp.int32)
    swap = [(0, 1), (1, 0)]
    plan = plan_of(n_dom)

    def place_fn(slots, at_ref):
        if plan is None:
            return slots
        step, early, late = plan
        owner, row = split_index(slots, per)
        distance = owner ^ at_ref[0]
        rank = jnp.full_like(slots, -2 * n_dom)
        for number, base in enumerate(early + late):
            rank = jnp.where(distance == base ^ (step * at_ref[1]), number, rank)
        return rank * per + row

    if plan is not None:
        their_table = lax.ppermute(table, "mp", swap)
    asked = lax.all_to_all(requests[0], "dom", split_axis=0, concat_axis=0, tiled=True)

    widths = [n_dom * per] if plan is None else [len(part) * per for part in plan[1:]]
    if plan is not None:
        near_a, their_table = lax.optimization_barrier((near_a, their_table))
    counts = count_matrices(near_a.T, self_a[None], count_a[None], where, place_fn, widths)
    (counts_b,) = count_matrices(
        near_b.T, self_b[None], count_b[None], where, lambda value, _: value, [near_a.shape[0]]
    )

    if plan is None:
        found = table.at[asked].get(mode="promise_in_bounds")
        moved = lax.all_to_all(found, "dom", split_axis=0, concat_axis=0, tiled=True)
        early, late = [], [moved.reshape(-1, features)]
    else:
        step = plan[0]
        found = {}
        for bases in BATCHES:
            picked = pick_rows(asked, where, table, their_table, bases, step)
            found.update(zip(bases, picked))

        def trade(base):
            pairs = [
                (2 * i + c, 2 * (i ^ (base ^ (step * c))) + c) for i in range(n_dom) for c in range(2)
            ]
            return lax.ppermute(found[base], ("dom", "mp"), pairs)

        early = [trade(base) for base in plan[1]]
        late = [trade(base) for base in plan[2]]

    their_a = lax.ppermute(weight_a, "mp", swap)
    their_b = lax.ppermute(weight_b, "mp", swap)
    count_line = count_a[None]
    before = None
    if early:
        early, (their_a, their_b, counts_b) = lax.optimization_barrier((early, (their_a, their_b, counts_b)))
        before = first_layer(counts[0], count_line, early, core_line, weight_a, their_a)
    own = first_layer(counts[-1], count_line, late, core_line, weight_a, their_a, before, last=True)
    other = lax.ppermute(own, "mp", swap)
    return second_layer(
        own, other, bias_a[None], counts_b, count_b[None], core_line, weight_b, their_b, bias_b.reshape(2, half)
    )


def solution(mesh):
    placed = (
        P("dom", "mp"),
        P(None, "mp"),
        P(),
        P(None, "mp"),
        P(),
        P("dom", None, None),
        P("dom", None),
        P("dom"),
        P("dom"),
        P("dom", None),
        P("dom"),
        P("dom"),
    )
    n_dom = mesh.shape["dom"]
    return jax.shard_map(
        functools.partial(shards, n_dom),
        mesh=mesh,
        in_specs=placed,
        out_specs=P("dom", "mp"),
        check_vma=False,
    )
```

```python
import functools

import jax
import jax.numpy as jnp
from jax import lax
from jax.experimental import pallas as pl
from jax.experimental.pallas import tpu as pltpu
from jax.sharding import PartitionSpec as P


LANES = 128
TAIL = 4
PICK = 4096
BATCHES = ((8, 13), (0, 1, 4, 5, 9, 12))


def split_index(value, size):
    if size & (size - 1) == 0:
        return lax.shift_right_logical(value, size.bit_length() - 1), value & (size - 1)
    quotient = lax.div(value, size)
    return quotient, value - quotient * size


def estimate(flops):
    return pl.CostEstimate(flops=flops, bytes_accessed=10**7, transcendentals=0)


def count_matrices(near, own, count, me, place_fn, widths):
    fan, total = near.shape
    block = min(2 * LANES, total)
    bits = max(1, fan.bit_length())
    fields = 32 // bits
    tall = min(LANES // 2, min(widths))

    def body(me_ref, near_ref, own_ref, count_ref, *outs):
        pieces = [(ref, at) for ref in outs for at in range(ref.shape[1] // LANES)]
        words = -(-len(pieces) // fields)
        rank = lax.broadcasted_iota(jnp.int32, (fan, LANES), 0)
        for lane in range(block // LANES):
            cols = slice(lane * LANES, (lane + 1) * LANES)
            place = place_fn(near_ref[:, cols], me_ref)
            group, low = split_index(place, LANES)
            word, field = split_index(group, fields)
            unit = jnp.left_shift(jnp.ones_like(field), field * bits)
            unit = jnp.where((rank < count_ref[:, cols]) & (place >= 0), unit, 0)
            units = [jnp.where(word == w, unit, 0) for w in range(words)]
            mine = place_fn(own_ref[:, cols], me_ref)
            for top in range(0, LANES, tall):
                rows = lax.broadcasted_iota(jnp.int32, (tall, LANES), 0) + top
                sums = [jnp.zeros((tall, LANES), jnp.int32) for _ in range(words)]
                for j in range(fan):
                    hit = rows == low[j : j + 1, :]
                    for w in range(words):
                        sums[w] = sums[w] + jnp.where(hit, units[w][j : j + 1, :], 0)
                for number, (ref, part) in enumerate(pieces):
                    found = lax.shift_right_logical(sums[number // fields], bits * (number % fields))
                    found = (found & ((1 << bits) - 1)).astype(jnp.float32)
                    here = slice(part * LANES + top, part * LANES + top + tall)
                    ref[0, here, cols] = found.astype(jnp.bfloat16)
                    one = jnp.where(rows == mine - number * LANES, 1.0, 0.0)
                    ref[1, here, cols] = one.astype(jnp.bfloat16)

    line = pl.BlockSpec((1, block), lambda i: (0, i))
    return pl.pallas_call(
        body,
        grid=(total // block,),
        in_specs=[
            pl.BlockSpec(memory_space=pltpu.SMEM),
            pl.BlockSpec((fan, block), lambda i: (0, i)),
            line,
            line,
        ],
        out_specs=[pl.BlockSpec((2, width, block), lambda i: (0, 0, i)) for width in widths],
        out_shape=[jax.ShapeDtypeStruct((2, width, total), jnp.bfloat16) for width in widths],
        compiler_params=pltpu.CompilerParams(vmem_limit_bytes=None),
        cost_estimate=estimate(10**9),
    )(me, near, own, count)


def pick_rows(asked, where, table, their_table, distances, step):
    nodes, share = table.shape
    per = asked.shape[1]
    block = min(PICK, nodes)
    total = len(distances) * per

    def body(at_ref, ask_ref, mine_ref, their_ref, *refs):
        outs, acc, ids = refs[:-2], refs[-2], refs[-1]
        now = pl.program_id(0)

        @pl.when(now == 0)
        def _():
            acc[...] = jnp.zeros_like(acc)
            for number, base in enumerate(distances):
                partner = at_ref[0] ^ (base ^ (step * at_ref[1]))
                line = ask_ref[pl.ds(partner, 1), :]
                ids[number * per : (number + 1) * per, :] = jnp.broadcast_to(line, (LANES, per)).T

        lanes = lax.broadcasted_iota(jnp.int32, (total, LANES), 1) + now * block
        wanted = ids[...]
        marks = [
            jnp.where(wanted - at == lanes, 1.0, 0.0).astype(jnp.bfloat16) for at in range(0, block, LANES)
        ]
        marks = jnp.concatenate(marks, axis=1)
        table_rows = jnp.concatenate([mine_ref[...], their_ref[...]], axis=1)
        acc[...] += jnp.dot(marks, table_rows, preferred_element_type=jnp.float32)

        @pl.when(now == pl.num_programs(0) - 1)
        def _():
            for number, ref in enumerate(outs):
                ref[...] = acc[number * per : (number + 1) * per, :].astype(jnp.bfloat16)

    rows = pl.BlockSpec((block, share), lambda i: (i, 0))
    return pl.pallas_call(
        body,
        grid=(nodes // block,),
        in_specs=[
            pl.BlockSpec(memory_space=pltpu.SMEM),
            pl.BlockSpec(asked.shape, lambda i: (0, 0)),
            rows,
            rows,
        ],
        out_specs=[pl.BlockSpec((per, 2 * share), lambda i: (0, 0))] * len(distances),
        out_shape=[jax.ShapeDtypeStruct((per, 2 * share), jnp.bfloat16)] * len(distances),
        scratch_shapes=[pltpu.VMEM((total, 2 * share), jnp.float32), pltpu.VMEM((total, LANES), jnp.int32)],
        compiler_params=pltpu.CompilerParams(vmem_limit_bytes=32 * 2**20),
        cost_estimate=estimate(4 * total * nodes * share),
    )(where, asked, table, their_table)


def first_layer(counts, count, rows, core, weight, their_weight, before=None, last=False):
    _, width, total = counts.shape
    cols = rows[0].shape[1]
    features, half = weight.shape[0] // 2, weight.shape[1]
    share = cols if cols < features else features // 2
    block = min(8 * LANES, total)
    have = before is not None

    def body(core_ref, c_ref, n_ref, *refs):
        refs = list(refs)
        row_refs = [refs.pop(0) for _ in rows]
        shard_refs = (refs.pop(0), refs.pop(0))
        old_ref = refs.pop(0) if have else None
        o_ref, turned = refs

        @pl.when(pl.program_id(0) == 0)
        def _():
            core_value = core_ref[0]
            first = pl.multiple_of(core_value * share, LANES)
            second = pl.multiple_of((1 - core_value) * share, LANES)
            spots = (first, second) if cols > share else (first,)
            value = jnp.concatenate([ref[...] for ref in row_refs], axis=0)
            for number, ref in enumerate(shard_refs):
                hidden_at = core_value * half if number == 0 else (1 - core_value) * half
                here = pl.ds(pl.multiple_of(hidden_at, LANES), half)
                for part in range(2):
                    pieces = [ref[pl.ds(part * features + at, share), :] for at in spots]
                    piece = jnp.concatenate(pieces, axis=0)
                    product = jnp.dot(value, piece, preferred_element_type=jnp.float32)
                    turned[part, here, :] = product.astype(jnp.bfloat16).T

        out = jnp.dot(turned[1], c_ref[0], preferred_element_type=jnp.float32)
        out = out * (1.0 / n_ref[...].astype(jnp.float32))
        out = out + jnp.dot(turned[0], c_ref[1], preferred_element_type=jnp.float32)
        if have:
            out = out + old_ref[...]
        o_ref[...] = out.astype(o_ref.dtype)

    out_spec = pl.BlockSpec((2 * half, block), lambda i: (0, i))
    specs = [
        pl.BlockSpec(memory_space=pltpu.SMEM),
        pl.BlockSpec((2, width, block), lambda i: (0, 0, i)),
        pl.BlockSpec((1, block), lambda i: (0, i)),
    ]
    specs += [pl.BlockSpec(piece.shape, lambda i: (0, 0)) for piece in rows]
    specs += [pl.BlockSpec(weight.shape, lambda i: (0, 0))] * 2
    operands = [core, counts, count, *rows, weight, their_weight]
    if have:
        specs.append(out_spec)
        operands.append(before)
    return pl.pallas_call(
        body,
        grid=(total // block,),
        in_specs=specs,
        out_specs=out_spec,
        out_shape=jax.ShapeDtypeStruct((2 * half, total), jnp.bfloat16 if last else jnp.float32),
        scratch_shapes=[pltpu.VMEM((2, 2 * half, width), jnp.bfloat16)],
        compiler_params=pltpu.CompilerParams(vmem_limit_bytes=32 * 2**20),
        cost_estimate=estimate(4 * width * total * cols),
    )(*operands)


def second_layer(own, other, bias_a, counts, count, core, weight, their_weight, bias_b):
    hidden, hops = own.shape
    half = hidden // 2
    seeds = counts.shape[2]
    block = min(TAIL * LANES, hops)

    def body(core_ref, own_ref, other_ref, ba_ref, c_ref, n_ref, w_ref, t_ref, bb_ref, o_ref, acc, bias):
        now = pl.program_id(0)

        @pl.when(now == 0)
        def _():
            bias[...] = jnp.broadcast_to(ba_ref[...], (LANES, hidden)).T
            acc[...] = jnp.zeros_like(acc)

        value = own_ref[...].astype(jnp.float32) + other_ref[...].astype(jnp.float32) + bias[:, :1]
        value = jnp.maximum(value, 0.0).astype(jnp.bfloat16)
        acc[0] += jnp.dot(value, c_ref[0], preferred_element_type=jnp.float32)
        acc[1] += jnp.dot(value, c_ref[1], preferred_element_type=jnp.float32)

        @pl.when(now == pl.num_programs(0) - 1)
        def _():
            self_b = acc[1].astype(jnp.bfloat16).T
            mean_b = (acc[0] * (1.0 / n_ref[...].astype(jnp.float32))).astype(jnp.bfloat16).T

            def state_of(ref, index):
                state = jnp.dot(self_b, ref[:hidden, :], preferred_element_type=jnp.float32)
                state = state + jnp.dot(mean_b, ref[hidden:, :], preferred_element_type=jnp.float32)
                return jnp.maximum(state + bb_ref[pl.ds(index, 1), :], 0.0)

            state = state_of(w_ref, core_ref[0])
            theirs = state_of(t_ref, 1 - core_ref[0])
            squares = jnp.sum(state * state + theirs * theirs, axis=1, keepdims=True)
            scale = jnp.sqrt(jnp.float32(hidden)) / jnp.sqrt(squares + hidden)
            o_ref[...] = (state * scale).astype(jnp.bfloat16)

    share = pl.BlockSpec((hidden, block), lambda i: (0, i))
    whole = [pl.BlockSpec(value.shape, lambda i: (0, 0)) for value in (count, weight, their_weight, bias_b)]
    return pl.pallas_call(
        body,
        grid=(hops // block,),
        in_specs=[
            pl.BlockSpec(memory_space=pltpu.SMEM),
            share,
            share,
            pl.BlockSpec(bias_a.shape, lambda i: (0, 0)),
            pl.BlockSpec((2, block, seeds), lambda i: (0, i, 0)),
            *whole,
        ],
        out_specs=pl.BlockSpec((seeds, half), lambda i: (0, 0)),
        out_shape=jax.ShapeDtypeStruct((seeds, half), jnp.bfloat16),
        scratch_shapes=[pltpu.VMEM((2, hidden, seeds), jnp.float32), pltpu.VMEM((hidden, LANES), jnp.float32)],
        cost_estimate=estimate(10**9),
        name="second_layer",
    )(core, own, other, bias_a, counts, count, weight, their_weight, bias_b)


def plan_of(n_dom):
    if n_dom != 16:
        return None
    return n_dom // 8, (8, 13, 0), (1, 4, 5, 9, 12)


def shards(
    n_dom,
    table,
    weight_a,
    bias_a,
    weight_b,
    bias_b,
    requests,
    near_a,
    self_a,
    count_a,
    near_b,
    self_b,
    count_b,
):
    features = table.shape[1]
    half = weight_a.shape[1]
    per = requests.shape[2]
    me = lax.axis_index("dom")
    core = lax.axis_index("mp")
    core_line = core.reshape(1).astype(jnp.int32)
    where = jnp.stack([me, core]).astype(jnp.int32)
    swap = [(0, 1), (1, 0)]
    plan = plan_of(n_dom)

    def place_fn(slots, at_ref):
        if plan is None:
            return slots
        step, early, late = plan
        owner, row = split_index(slots, per)
        distance = owner ^ at_ref[0]
        rank = jnp.full_like(slots, -2 * n_dom)
        for number, base in enumerate(early + late):
            rank = jnp.where(distance == base ^ (step * at_ref[1]), number, rank)
        return rank * per + row

    if plan is not None:
        their_table = lax.ppermute(table, "mp", swap)
    asked = lax.all_to_all(requests[0], "dom", split_axis=0, concat_axis=0, tiled=True)

    widths = [n_dom * per] if plan is None else [len(part) * per for part in plan[1:]]
    if plan is not None:
        near_a, their_table = lax.optimization_barrier((near_a, their_table))
    counts = count_matrices(near_a.T, self_a[None], count_a[None], where, place_fn, widths)
    (counts_b,) = count_matrices(
        near_b.T, self_b[None], count_b[None], where, lambda value, _: value, [near_a.shape[0]]
    )

    if plan is None:
        found = table.at[asked].get(mode="promise_in_bounds")
        moved = lax.all_to_all(found, "dom", split_axis=0, concat_axis=0, tiled=True)
        early, late = [], [moved.reshape(-1, features)]
    else:
        step = plan[0]
        found = {}
        for bases in BATCHES:
            picked = pick_rows(asked, where, table, their_table, bases, step)
            found.update(zip(bases, picked))

        def trade(base):
            pairs = [
                (2 * i + c, 2 * (i ^ (base ^ (step * c))) + c) for i in range(n_dom) for c in range(2)
            ]
            return lax.ppermute(found[base], ("dom", "mp"), pairs)

        early = [trade(base) for base in plan[1]]
        late = [trade(base) for base in plan[2]]

    their_a = lax.ppermute(weight_a, "mp", swap)
    their_b = lax.ppermute(weight_b, "mp", swap)
    count_line = count_a[None]
    before = None
    if early:
        early, (their_a, their_b, counts_b) = lax.optimization_barrier((early, (their_a, their_b, counts_b)))
        before = first_layer(counts[0], count_line, early, core_line, weight_a, their_a)
    own = first_layer(counts[-1], count_line, late, core_line, weight_a, their_a, before, last=True)
    other = lax.ppermute(own, "mp", swap)
    return second_layer(
        own, other, bias_a[None], counts_b, count_b[None], core_line, weight_b, their_b, bias_b.reshape(2, half)
    )


def solution(mesh):
    placed = (
        P("dom", "mp"),
        P(None, "mp"),
        P(),
        P(None, "mp"),
        P(),
        P("dom", None, None),
        P("dom", None),
        P("dom"),
        P("dom"),
        P("dom", None),
        P("dom"),
        P("dom"),
    )
    n_dom = mesh.shape["dom"]
    return jax.shard_map(
        functools.partial(shards, n_dom),
        mesh=mesh,
        in_specs=placed,
        out_specs=P("dom", "mp"),
        check_vma=False,
    )
```
